32 devices in a mesh: dp: 4 (over y, core), tensor: 8 (over z, x).
Axes of the slice: x: 2, y: 2, z: 4, core: 2. Of those that a mesh axis runs over, the one named last changes fastest.
Arguments:
- ref_hidden: bfloat16 [1152, 4608], P('dp', 'tensor'), may hold values from -6 to 6
- pol_hidden: bfloat16 [1152, 4608], P('dp', 'tensor'), may hold values from -6 to 6
- readout: bfloat16 [1152, 4608], P('dp', 'tensor'), may hold values from -0.019897461 to 0.019897461
- lengths: int32 [12], P('dp'), may hold values from 16 to 96, as said below
- pairing: int32 [12], replicated, may hold values from 0 to 11, each once
- pre_gain: float32 [4608], replicated, may hold values from 0.25 to 1.75
- post_gain: float32 [4608], replicated, may hold values from 0.25 to 1.75
- w_query: bfloat16 [4608, 4096], P('dp', 'tensor'), may hold values from -0.09375 to 0.09375
- w_key: bfloat16 [4608, 2048], P('dp', 'tensor'), may hold values from -3 to 3
- value_projection: bfloat16 [4608, 2048], P('dp', 'tensor'), may hold values from -0.09375 to 0.09375
- w_out: bfloat16 [4608, 4096], P('dp', 'tensor'), may hold values from -0.09375 to 0.09375
- a_query: bfloat16 [4608, 64], P('dp'), may hold values from -0.09375 to 0.09375
- a_value: bfloat16 [4608, 64], P('dp'), may hold values from -0.09375 to 0.09375
- query_second_factor: bfloat16 [64, 4096], P(None, 'tensor'), may hold values from -0.75 to 0.75
- value_second_factor: bfloat16 [64, 2048], P(None, 'tensor'), may hold values from -0.75 to 0.75
Outputs:
- policy_out: bfloat16 [1152, 4608], P('dp', 'tensor')
- reference_out: bfloat16 [1152, 4608], P('dp', 'tensor')
- dpo_loss: float32 [], replicated
- grad_hidden: bfloat16 [1152, 4608], P('dp', 'tensor')
- grad_a: float32 [4608, 128], P('dp')
- query_factor_gradient: float32 [64, 4096], P(None, 'tensor')
- value_factor_gradient: float32 [64, 2048], P(None, 'tensor')
The draws below stay inside these ranges and needn't reach their ends.
Inputs may be any that keep to these rules, and one draw needn't show every extreme that they name: `lengths`: every sequence has at least one valid token and some sequence is full. `pairing`: entries 2k and 2k + 1 name the chosen and the rejected sequence of pair k; every sequence appears once.
All inputs are finite; a program needn't handle non-finite values.
Results may differ from the reference program's by a relative error of at most 0.0233.
The reference program's roundings to bfloat16 on the way count: a program that leaves them out, or rounds other values in their place, can miss the bound.
Values may be sent and summed in bfloat16 or wider, within the bound.
A program may use at most 128 MiB of HBM per device.

```python
import jax
import jax.numpy as jnp
from jax import lax

MODEL_WIDTH = 4608
HQ = 32
KEY_VALUE_HEADS = 16
HEAD_SIZE = 128
ADAPTER_RANK = 64
SEQUENCE_SLOTS = 96
SEQUENCE_COUNT = 12
TOKEN_SLOTS = 1152
N_TENSOR = 8


def draw_lengths(key, part):
    first_key = jax.random.fold_in(key, 11)
    second_key = jax.random.fold_in(key, 12)
    lowest = max(1, SEQUENCE_SLOTS // 6)
    drawn = jax.random.randint(first_key, (SEQUENCE_COUNT,), lowest, SEQUENCE_SLOTS + 1)
    target_row = jax.random.randint(second_key, (), 0, SEQUENCE_COUNT)
    return jnp.where(jnp.arange(SEQUENCE_COUNT) == target_row, SEQUENCE_SLOTS, drawn).astype(jnp.int32)


def key_head_scales(scale_random_key, lowest, highest):
    uniform_sample = jax.random.uniform(scale_random_key, (KEY_VALUE_HEADS,), jnp.float32)
    spread_heads = jnp.exp(jnp.log(lowest) + uniform_sample * (jnp.log(highest) - jnp.log(lowest)))
    return (spread_heads[:, None] * jnp.ones((1, HEAD_SIZE), jnp.float32)).reshape(KEY_VALUE_HEADS * HEAD_SIZE)


def draw_w_key(key, part):
    scale_random_key = jax.random.fold_in(key, 21)
    entry_random_key = jax.random.fold_in(key, 22)
    spread_heads = key_head_scales(scale_random_key, 1.0, 8.0)
    table_entries = jax.random.truncated_normal(entry_random_key, -3.0, 3.0, (MODEL_WIDTH, KEY_VALUE_HEADS * HEAD_SIZE), jnp.float32)
    return (table_entries * spread_heads[None, :] * float(MODEL_WIDTH) ** (-0.5)).astype(jnp.bfloat16)


def steps_of(own_key, dims, cuts, least, high):
    level = 1.0
    for dim, parts in cuts:
        steps = jax.random.uniform(jax.random.fold_in(jax.random.fold_in(own_key, 6), dim), (parts,), jnp.float32, least / len(cuts), high / len(cuts))
        level = level * jnp.repeat(jnp.exp(steps), dims[dim] // parts).reshape((-1,) + (1,) * (len(dims) - 1 - dim))
    return level


def gaussian(key, extent, deviation, limit, split=(), kind=jnp.bfloat16):
    entries = deviation * jax.random.normal(key, extent, jnp.float32)
    if split:
        entries = entries * steps_of(key, extent, split, -0.22, 0.18)
    return jnp.clip(entries, -limit, limit).astype(kind)


def setup_inputs(seed: int = 0) -> dict:
    splits = jax.random.split(jax.random.key(seed), 16)
    return {
        "ref_hidden": gaussian(splits[0], (TOKEN_SLOTS, MODEL_WIDTH), 1.0, 6.0, ((0, 4), (1, 8))),
        "pol_hidden": gaussian(splits[1], (TOKEN_SLOTS, MODEL_WIDTH), 1.0, 6.0, ((0, 4), (1, 8))),
        "readout": gaussian(splits[2], (TOKEN_SLOTS, MODEL_WIDTH), 0.003, 0.019897461, ((0, 4), (1, 8))),
        "lengths": draw_lengths(jax.random.fold_in(splits[15], 71), 0),
        "pairing": jax.random.permutation(splits[4], SEQUENCE_COUNT).astype(jnp.int32),
        "pre_gain": jnp.clip(1.0 + 0.15 * jax.random.normal(splits[5], (MODEL_WIDTH,), jnp.float32), 0.25, 1.75),
        "post_gain": jnp.clip(1.0 + 0.15 * jax.random.normal(splits[6], (MODEL_WIDTH,), jnp.float32), 0.25, 1.75),
        "w_query": gaussian(splits[7], (MODEL_WIDTH, HQ * HEAD_SIZE), MODEL_WIDTH ** -0.5, 0.09375, ((0, 4), (1, 8))),
        "w_key": draw_w_key(jax.random.fold_in(splits[15], 71), 0),
        "value_projection": gaussian(splits[9], (MODEL_WIDTH, KEY_VALUE_HEADS * HEAD_SIZE), MODEL_WIDTH ** -0.5, 0.09375, ((0, 4), (1, 8))),
        "w_out": gaussian(splits[10], (MODEL_WIDTH, HQ * HEAD_SIZE), (HQ * HEAD_SIZE) ** -0.5, 0.09375, ((0, 4), (1, 8))),
        "a_query": gaussian(splits[11], (MODEL_WIDTH, ADAPTER_RANK), MODEL_WIDTH ** -0.5, 0.09375, ((0, 4),)),
        "a_value": gaussian(splits[12], (MODEL_WIDTH, ADAPTER_RANK), MODEL_WIDTH ** -0.5, 0.09375, ((0, 4),)),
        "query_second_factor": gaussian(splits[13], (ADAPTER_RANK, HQ * HEAD_SIZE), ADAPTER_RANK ** -0.5, 0.75, ((1, 8),)),
        "value_second_factor": gaussian(splits[14], (ADAPTER_RANK, KEY_VALUE_HEADS * HEAD_SIZE), ADAPTER_RANK ** -0.5, 0.75, ((1, 8),)),
    }


NORM_EPS = 1e-06
SOFT_CAP = 50.0
ADAPTER_SCALE = 0.5
DPO_BETA = 0.5
LOSS_SCALE = 256.0
ROPE_BASE = 10000.0

def query_scale():
    return float(MODEL_WIDTH // HQ) ** (-0.5)

def apply_rotation(value_rows, direction):
    length = value_rows.shape[1]
    head_depth = value_rows.shape[3]
    middle = head_depth // 2
    spacing = ROPE_BASE ** (-2.0 * jnp.arange(middle, dtype=jnp.float32) / head_depth)
    angles = jnp.arange(length, dtype=jnp.float32)[:, None] * spacing[None, :]
    cosine = jnp.cos(angles)[None, :, None, :]
    sine_part = direction * jnp.sin(angles)[None, :, None, :]
    leading = value_rows[..., :middle]
    trailing = value_rows[..., middle:]
    return jnp.concatenate([leading * cosine - trailing * sine_part, trailing * cosine + leading * sine_part], axis=-1)

def allowed_mask(lengths, length):
    places = jnp.arange(length)
    causal = places[None, :] <= places[:, None]
    living = places[None, :] < lengths[:, None]
    return causal[None, None, None, :, :] & living[:, None, None, None, :]

def attend(query_rows, rotated_keys, value_rows, lengths):
    seqs_here, length, q_heads, head_depth = query_rows.shape
    kv_heads = rotated_keys.shape[2]
    grouped_heads = query_rows.reshape(seqs_here, length, kv_heads, q_heads // kv_heads, head_depth)
    scores = jnp.einsum('sqkgd,spkd->skgqp', grouped_heads.astype(jnp.float32), rotated_keys.astype(jnp.float32)) * query_scale()
    capped = SOFT_CAP * jnp.tanh(scores / SOFT_CAP)
    allowed = allowed_mask(lengths, length)
    weights = jnp.where(allowed, jnp.exp(capped), 0.0)
    probabilities = weights / lax.optimization_barrier(jnp.sum(weights, axis=-1, keepdims=True))
    probs_low = probabilities.astype(jnp.bfloat16)
    mixed_out = jnp.einsum('skgqp,spkd->sqkgd', probs_low.astype(jnp.float32), value_rows.astype(jnp.float32))
    return (mixed_out.astype(jnp.bfloat16).reshape(seqs_here, length, q_heads, head_depth), probs_low, probabilities, capped)

def attend_back(grad_mixed, query_rows, rotated_keys, value_rows, probs_low, probabilities, capped):
    seqs_here, length, q_heads, head_depth = query_rows.shape
    kv_heads = rotated_keys.shape[2]
    shape_five = (seqs_here, length, kv_heads, q_heads // kv_heads, head_depth)
    grouped_heads = query_rows.reshape(shape_five).astype(jnp.float32)
    grad_grouped = grad_mixed.reshape(shape_five).astype(jnp.float32)
    grad_probs = jnp.einsum('sqkgd,spkd->skgqp', grad_grouped, value_rows.astype(jnp.float32))
    value_rows_gradient = jnp.einsum('skgqp,sqkgd->spkd', probs_low.astype(jnp.float32), grad_grouped)
    centered = grad_probs - lax.optimization_barrier(jnp.sum(grad_probs * probabilities, axis=-1, keepdims=True))
    grad_scores = (probabilities * centered * (1.0 - (capped / SOFT_CAP) ** 2) * query_scale()).astype(jnp.bfloat16)
    grad_scores = grad_scores.astype(jnp.float32)
    query_rows_gradient = jnp.einsum('skgqp,spkd->sqkgd', grad_scores, rotated_keys.astype(jnp.float32)).reshape(seqs_here, length, q_heads, head_depth)
    key_rows_gradient = jnp.einsum('skgqp,sqkgd->spkd', grad_scores, grouped_heads)
    return (query_rows_gradient, key_rows_gradient, value_rows_gradient)

def normalize(hidden, gain):
    wide_rows = hidden.astype(jnp.float32)
    pre_scale = lax.rsqrt(lax.optimization_barrier(jnp.sum(wide_rows * wide_rows, axis=1, keepdims=True)) / MODEL_WIDTH + NORM_EPS)
    return ((wide_rows * pre_scale * gain).astype(jnp.bfloat16), pre_scale)

def attention_layer(hidden, normed, lengths, post_gain, w_query, w_key, value_projection, w_out, adapters):
    query_rows = jnp.dot(normed, w_query, preferred_element_type=jnp.float32)
    keys_before_rotation = jnp.dot(normed, w_key, preferred_element_type=jnp.float32)
    value_rows = jnp.dot(normed, value_projection, preferred_element_type=jnp.float32)
    low_rank_update = None
    if adapters is not None:
        a_query, a_value, query_second_factor, value_second_factor = adapters
        low_rank_update = jnp.dot(normed, jnp.concatenate([a_query, a_value], axis=1), preferred_element_type=jnp.float32).astype(jnp.bfloat16)
        query_rows = query_rows + ADAPTER_SCALE * jnp.dot(low_rank_update[:, :ADAPTER_RANK], query_second_factor, preferred_element_type=jnp.float32)
        value_rows = value_rows + ADAPTER_SCALE * jnp.dot(low_rank_update[:, ADAPTER_RANK:], value_second_factor, preferred_element_type=jnp.float32)
    query_rows = apply_rotation(query_rows.reshape(SEQUENCE_COUNT, SEQUENCE_SLOTS, HQ, HEAD_SIZE), 1.0).astype(jnp.bfloat16)
    rotated_keys = apply_rotation(keys_before_rotation.reshape(SEQUENCE_COUNT, SEQUENCE_SLOTS, KEY_VALUE_HEADS, HEAD_SIZE), 1.0).astype(jnp.bfloat16)
    value_rows = value_rows.reshape(SEQUENCE_COUNT, SEQUENCE_SLOTS, KEY_VALUE_HEADS, HEAD_SIZE).astype(jnp.bfloat16)
    mixed_out, probs_low, probabilities, capped = attend(query_rows, rotated_keys, value_rows, lengths)
    flat_mixed = mixed_out.reshape(TOKEN_SLOTS, HQ * HEAD_SIZE)
    group_cols = HQ * HEAD_SIZE // N_TENSOR
    contract_cols = (((1,), (1,)), ((), ()))

    def add_group(index_g, running):
        start = (index_g * group_cols).astype(jnp.int32)
        columns = lax.dynamic_slice_in_dim(flat_mixed, start, group_cols, 1)
        w_columns = lax.dynamic_slice_in_dim(w_out, start, group_cols, 1)
        term_low = lax.dot_general(columns, w_columns, contract_cols, preferred_element_type=jnp.float32).astype(jnp.bfloat16)
        return running + lax.optimization_barrier(term_low).astype(jnp.float32)
    summed = lax.fori_loop(jnp.int32(0), jnp.int32(N_TENSOR), add_group, jnp.zeros((TOKEN_SLOTS, MODEL_WIDTH), jnp.float32))
    post_scale = lax.rsqrt(lax.optimization_barrier(jnp.sum(summed * summed, axis=1, keepdims=True)) / MODEL_WIDTH + NORM_EPS)
    result = hidden.astype(jnp.float32) + summed * post_scale * post_gain
    saved = (low_rank_update, query_rows, rotated_keys, value_rows, probs_low, probabilities, capped, summed, post_scale)
    return (result, saved)

def block_hook(grads, factor):
    grouped_heads = grads.astype(jnp.float32).reshape(TOKEN_SLOTS, N_TENSOR, -1)
    grouped_factors = factor.astype(jnp.float32).reshape(ADAPTER_RANK, N_TENSOR, -1)
    split_pieces = (ADAPTER_SCALE * jnp.einsum('fei,kei->fek', grouped_heads, grouped_factors)).astype(jnp.bfloat16)
    return lax.optimization_barrier(jnp.sum(lax.optimization_barrier(split_pieces).astype(jnp.float32), axis=1))

def reference(ref_hidden, pol_hidden, readout, lengths, pairing, pre_gain, post_gain, w_query, w_key, value_projection, w_out, a_query, a_value, query_second_factor, value_second_factor):
    ref_normed, ref_scale = normalize(ref_hidden, pre_gain)
    ref_result, ref_saved = attention_layer(ref_hidden, ref_normed, lengths, post_gain, w_query, w_key, value_projection, w_out, None)
    pol_normed, pol_scale = normalize(pol_hidden, pre_gain)
    pol_result, pol_saved = attention_layer(pol_hidden, pol_normed, lengths, post_gain, w_query, w_key, value_projection, w_out, (a_query, a_value, query_second_factor, value_second_factor))
    readout_wide = readout.astype(jnp.float32)
    living = (jnp.arange(SEQUENCE_SLOTS)[None, :] < lengths[:, None]).astype(jnp.float32)

    def sequence_score(result):
        return lax.optimization_barrier(jnp.sum(lax.optimization_barrier(jnp.sum(result * readout_wide, axis=1)).reshape(SEQUENCE_COUNT, SEQUENCE_SLOTS) * living, axis=1))
    ratios = sequence_score(pol_result) - sequence_score(ref_result)
    chosen = pairing[0::2]
    rejected = pairing[1::2]
    margins = DPO_BETA * (ratios[chosen] - ratios[rejected])
    dpo_loss = jnp.sum(jax.nn.softplus(-margins))
    pair_pull = DPO_BETA * LOSS_SCALE * jax.nn.sigmoid(-margins)
    coefficients = jnp.zeros((SEQUENCE_COUNT,), jnp.float32).at[chosen].add(-pair_pull).at[rejected].add(pair_pull)
    grad_result = (coefficients[:, None] * living).reshape(TOKEN_SLOTS, 1) * readout_wide
    low_rank_update, query_rows, rotated_keys, value_rows, probs_low, probabilities, capped, summed, post_scale = pol_saved
    post_dot = lax.optimization_barrier(jnp.sum(summed * post_gain * grad_result, axis=1, keepdims=True))
    grad_summed = post_scale * post_gain * grad_result - summed * post_scale ** 3 * post_dot / MODEL_WIDTH
    grad_wide = grad_summed.astype(jnp.bfloat16)
    grad_mixed = jnp.dot(grad_wide, w_out, preferred_element_type=jnp.float32).astype(jnp.bfloat16)
    grad_q_rot, rotated_key_gradient, value_head_gradient = attend_back(grad_mixed.reshape(SEQUENCE_COUNT, SEQUENCE_SLOTS, HQ, HEAD_SIZE), query_rows, rotated_keys, value_rows, probs_low, probabilities, capped)
    query_rows_gradient = apply_rotation(grad_q_rot, -1.0).reshape(TOKEN_SLOTS, HQ * HEAD_SIZE).astype(jnp.bfloat16)
    key_rows_gradient = apply_rotation(rotated_key_gradient, -1.0).reshape(TOKEN_SLOTS, KEY_VALUE_HEADS * HEAD_SIZE).astype(jnp.bfloat16)
    value_rows_gradient = value_head_gradient.reshape(TOKEN_SLOTS, KEY_VALUE_HEADS * HEAD_SIZE).astype(jnp.bfloat16)
    rows_contraction = (((0,), (0,)), ((), ()))
    contract_cols = (((1,), (1,)), ((), ()))
    query_factor_gradient = ADAPTER_SCALE * lax.dot_general(low_rank_update[:, :ADAPTER_RANK], query_rows_gradient, rows_contraction, preferred_element_type=jnp.float32)
    value_factor_gradient = ADAPTER_SCALE * lax.dot_general(low_rank_update[:, ADAPTER_RANK:], value_rows_gradient, rows_contraction, preferred_element_type=jnp.float32)
    adapter_grad = jnp.concatenate([block_hook(query_rows_gradient, query_second_factor), block_hook(value_rows_gradient, value_second_factor)], axis=1)
    grad_a = lax.dot_general(pol_normed.astype(jnp.float32), adapter_grad, rows_contraction, precision=lax.Precision.HIGHEST)
    a_both = jnp.concatenate([a_query, a_value], axis=1).astype(jnp.float32)
    grad_normed = lax.dot_general(query_rows_gradient, w_query, contract_cols, preferred_element_type=jnp.float32)
    grad_normed = grad_normed + lax.dot_general(key_rows_gradient, w_key, contract_cols, preferred_element_type=jnp.float32)
    grad_normed = grad_normed + lax.dot_general(value_rows_gradient, value_projection, contract_cols, preferred_element_type=jnp.float32)
    grad_normed = grad_normed + lax.dot_general(adapter_grad, a_both, contract_cols, precision=lax.Precision.HIGHEST)
    narrow = pol_hidden.astype(jnp.float32)
    pre_dot = lax.optimization_barrier(jnp.sum(narrow * pre_gain * grad_normed, axis=1, keepdims=True))
    grad_hidden = grad_result + pol_scale * pre_gain * grad_normed - narrow * pol_scale ** 3 * pre_dot / MODEL_WIDTH
    return (pol_result.astype(jnp.bfloat16), ref_result.astype(jnp.bfloat16), dpo_loss, grad_hidden.astype(jnp.bfloat16), grad_a, query_factor_gradient, value_factor_gradient)
```

```python
import jax
import jax.numpy as jnp
from jax import lax
from jax.experimental import pallas as pl
from jax.experimental.pallas import tpu as pltpu
from jax.sharding import PartitionSpec as P

MODEL_WIDTH = 4608
HQ = 32
HEAD_SIZE = 128


NORM_EPS = 1e-06
SOFT_CAP = 50.0
ADAPTER_SCALE = 0.5
DPO_BETA = 0.5
LOSS_SCALE = 256.0
ROPE_BASE = 10000.0


def query_scale():
    return float(MODEL_WIDTH // HQ) ** (-0.5)


def apply_rotation(value_rows, direction):
    length = value_rows.shape[1]
    head_depth = value_rows.shape[3]
    middle = head_depth // 2
    spacing = ROPE_BASE ** (-2.0 * jnp.arange(middle, dtype=jnp.float32) / head_depth)
    angles = jnp.arange(length, dtype=jnp.float32)[:, None] * spacing[None, :]
    cosine = jnp.cos(angles)[None, :, None, :]
    sine_part = direction * jnp.sin(angles)[None, :, None, :]
    leading = value_rows[..., :middle]
    trailing = value_rows[..., middle:]
    return jnp.concatenate(
        [leading * cosine - trailing * sine_part, trailing * cosine + leading * sine_part], axis=-1
    )


def allowed_mask(lengths, length):
    places = jnp.arange(length)
    causal = places[None, :] <= places[:, None]
    living = places[None, :] < lengths[:, None]
    return causal[None, None, None, :, :] & living[:, None, None, None, :]


def attend(query_rows, rotated_keys, value_rows, lengths):
    seqs_here, length, q_heads, head_depth = query_rows.shape
    kv_heads = rotated_keys.shape[2]
    grouped_heads = query_rows.reshape(seqs_here, length, kv_heads, q_heads // kv_heads, head_depth)
    scores = (
        jnp.einsum(
            "sqkgd,spkd->skgqp", grouped_heads, rotated_keys, preferred_element_type=jnp.float32
        )
        * query_scale()
    )
    capped = SOFT_CAP * jnp.tanh(scores / SOFT_CAP)
    allowed = allowed_mask(lengths, length)
    weights = jnp.where(allowed, jnp.exp(capped), 0.0)
    probabilities = weights / jnp.sum(weights, axis=-1, keepdims=True)
    probs_low = probabilities.astype(jnp.bfloat16)
    mixed_out = jnp.einsum(
        "skgqp,spkd->sqkgd", probs_low, value_rows, preferred_element_type=jnp.float32
    )
    return (
        mixed_out.astype(jnp.bfloat16).reshape(seqs_here, length, q_heads, head_depth),
        probs_low,
        probabilities,
        capped,
    )


def attend_back(grad_mixed, query_rows, rotated_keys, value_rows, probs_low, probabilities, capped):
    seqs_here, length, q_heads, head_depth = query_rows.shape
    kv_heads = rotated_keys.shape[2]
    shape_five = (seqs_here, length, kv_heads, q_heads // kv_heads, head_depth)
    grouped_heads = query_rows.reshape(shape_five)
    grad_grouped = grad_mixed.reshape(shape_five)
    grad_probs = jnp.einsum(
        "sqkgd,spkd->skgqp", grad_grouped, value_rows, preferred_element_type=jnp.float32
    )
    value_rows_gradient = jnp.einsum(
        "skgqp,sqkgd->spkd", probs_low, grad_grouped, preferred_element_type=jnp.float32
    )
    centered = grad_probs - jnp.sum(grad_probs * probabilities, axis=-1, keepdims=True)
    grad_scores = (
        probabilities * centered * (1.0 - (capped / SOFT_CAP) ** 2) * query_scale()
    ).astype(jnp.bfloat16)
    query_rows_gradient = jnp.einsum(
        "skgqp,spkd->sqkgd", grad_scores, rotated_keys, preferred_element_type=jnp.float32
    ).reshape(seqs_here, length, q_heads, head_depth)
    key_rows_gradient = jnp.einsum(
        "skgqp,sqkgd->spkd", grad_scores, grouped_heads, preferred_element_type=jnp.float32
    )
    return (query_rows_gradient, key_rows_gradient, value_rows_gradient)


MESH = pl.DeviceIdType.MESH
VMEM_GRANT = 60 * 2**20


def grid_of(axis, count):
    if axis == "dp":
        inner = 2 if count % 2 == 0 else 1
    else:
        inner = 1
        while (inner * 2) ** 2 <= count and count % (inner * 2) == 0:
            inner *= 2
    return count // inner, inner


def row_chunk(rows):
    for size in (48, 32, 16):
        if rows % size == 0:
            return size
    return rows


class Place:
    def __init__(self, axis, count):
        self.axis = axis
        self.outer, self.inner = grid_of(axis, count)
        rank = lax.axis_index(axis)
        self.a = lax.div(rank, self.inner)
        self.b = lax.rem(rank, self.inner)
        self.rank = rank

    def out_at(self, j):
        return lax.rem(self.a + j + self.outer, self.outer)

    def in_at(self, k):
        return lax.rem(self.b + k + self.inner, self.inner)

    def slot(self, j, k):
        return self.out_at(j) * self.inner + self.in_at(k)

    def peers(self):
        return [self.slot(j, 0) for j in range(1, self.outer)] + [
            self.slot(0, k) for k in range(1, self.inner)
        ]


def remote(src, dst, send_sem, recv_sem, axis, rank):
    return pltpu.make_async_remote_copy(
        src_ref=src,
        dst_ref=dst,
        send_sem=send_sem,
        recv_sem=recv_sem,
        device_id={axis: rank},
        device_id_type=MESH,
    )


def communicate(name, number, counts, gathers=(), reduces=(), gain=None):
    places_used = sorted({axis for _, axis, _ in gathers} | ({"tensor"} if reduces else set()))
    tensor_count = counts["tensor"]
    operands, in_specs, out_shapes, out_specs, scratch = [], [], [], [], []
    vmem = pl.BlockSpec(memory_space=pltpu.VMEM)
    plan = []
    for array, axis, kind in gathers:
        operands.append(array)
        in_specs.append(vmem)
        whole = (counts[axis],) + array.shape
        outer, inner = grid_of(axis, counts[axis])
        entry = {"axis": axis, "kind": kind, "x": len(operands) - 1}
        if kind in ("vmem", "hbm"):
            entry["out"] = len(out_shapes)
            out_shapes.append(jax.ShapeDtypeStruct(whole, array.dtype))
            out_specs.append(vmem if kind == "vmem" else pl.BlockSpec(memory_space=pl.ANY))
        else:
            entry["held"] = len(scratch)
            scratch.append(pltpu.VMEM(whole, array.dtype))
            entry["out"] = len(out_shapes)
            out_shapes.append(
                jax.ShapeDtypeStruct((array.shape[0], array.shape[1] * counts[axis]), jnp.bfloat16)
            )
            out_specs.append(vmem)
            if kind == "norm":
                out_shapes.append(jax.ShapeDtypeStruct((array.shape[0], 1), jnp.float32))
                out_specs.append(vmem)
                entry["gain"] = len(operands)
                operands.append(gain.reshape(1, -1))
                in_specs.append(vmem)
        entry["sems"] = len(scratch)
        n_outer, n_inner = max(outer - 1, 1), max(outer * (inner - 1), 1)
        scratch += [
            pltpu.SemaphoreType.DMA((n_outer,)),
            pltpu.SemaphoreType.DMA((n_outer,)),
            pltpu.SemaphoreType.DMA((n_inner,)),
            pltpu.SemaphoreType.DMA((n_inner,)),
            pltpu.SemaphoreType.DMA,
        ]
        plan.append(entry)
    sums = []
    for array in reduces:
        rows, width = array.shape
        outer, inner = grid_of("tensor", tensor_count)
        part = width // tensor_count
        n_inner = max(outer * (inner - 1), 1)
        sums.append({"x": len(operands), "out": len(out_shapes), "scratch": len(scratch)})
        operands.append(array)
        in_specs.append(vmem)
        out_shapes.append(jax.ShapeDtypeStruct((rows, part), jnp.float32))
        out_specs.append(vmem)
        scratch += [
            pltpu.VMEM((tensor_count, rows, part), array.dtype),
            pltpu.VMEM((n_inner, rows, part), array.dtype),
            pltpu.VMEM((outer, rows, part), array.dtype),
            pltpu.VMEM((outer, rows, part), array.dtype),
            pltpu.SemaphoreType.DMA((n_inner,)),
            pltpu.SemaphoreType.DMA((n_inner,)),
            pltpu.SemaphoreType.DMA((outer,)),
            pltpu.SemaphoreType.DMA((outer,)),
        ]
    n_in, n_out = len(operands), len(out_shapes)

    def kernel(*refs):
        ins, outs, work = refs[:n_in], refs[n_in : n_in + n_out], refs[n_in + n_out :]
        places = {axis: Place(axis, counts[axis]) for axis in places_used}
        barrier = pltpu.get_barrier_semaphore()
        total = 0
        for axis, place in places.items():
            for peer in place.peers():
                pl.semaphore_signal(barrier, inc=1, device_id={axis: peer}, device_id_type=MESH)
                total += 1
        pl.semaphore_wait(barrier, total)
        for entry in plan:
            place = places[entry["axis"]]
            x = ins[entry["x"]]
            held = work[entry["held"]] if "held" in entry else outs[entry["out"]]
            so, ro, si, ri, own_sem = work[entry["sems"] : entry["sems"] + 5]
            entry["far"], entry["near"] = [], []
            mine = held.at[place.rank]
            for j in range(1, place.outer):
                copy = remote(
                    x, mine, so.at[j - 1], ro.at[j - 1], place.axis, place.slot(j, 0)
                )
                copy.start()
                entry["far"].append(copy)
            for k in range(1, place.inner):
                copy = remote(
                    x, mine, si.at[k - 1], ri.at[k - 1], place.axis, place.slot(0, k)
                )
                copy.start()
                entry["near"].append(copy)
            entry["own"] = pltpu.make_async_copy(x, mine, own_sem)
            entry["own"].start()
        for item in sums:
            place = places["tensor"]
            x = ins[item["x"]]
            stage, near_box, outgoing, far_box, si, ri, so, ro = work[
                item["scratch"] : item["scratch"] + 8
            ]
            part = stage.shape[2]
            rows = stage.shape[1]
            size = row_chunk(rows)

            @pl.loop(0, rows // size)
            def _(step, x=x, stage=stage, part=part, size=size):
                at = pl.ds(pl.multiple_of(step * size, size), size)
                for n in range(tensor_count):
                    stage[n, at, :] = x[at, n * part : (n + 1) * part]

            item["near"], item["far"] = {}, {}
            for j in [*range(1, place.outer), 0]:
                for k in range(1, place.inner):
                    at = j * (place.inner - 1) + k - 1
                    copy = remote(
                        stage.at[place.slot(j, k)],
                        near_box.at[at],
                        si.at[at],
                        ri.at[at],
                        "tensor",
                        place.slot(0, k),
                    )
                    copy.start()
                    item["near"][j, k] = copy
        for item in sums:
            place = places["tensor"]
            out = outs[item["out"]]
            stage, near_box, outgoing, far_box, si, ri, so, ro = work[
                item["scratch"] : item["scratch"] + 8
            ]
            rows = stage.shape[1]
            size = row_chunk(rows)
            for j in [*range(1, place.outer), 0]:
                for k in range(1, place.inner):
                    item["near"][j, k].wait_recv()

                @pl.loop(0, rows // size)
                def _(step, j=j):
                    at = pl.ds(pl.multiple_of(step * size, size), size)
                    value = stage[place.slot(j, 0), at, :].astype(jnp.float32)
                    for k in range(1, place.inner):
                        value += near_box[j * (place.inner - 1) + k - 1, at, :].astype(jnp.float32)
                    if j:
                        outgoing[j, at, :] = value.astype(outgoing.dtype)
                    else:
                        out[at, :] = value

                if j:
                    copy = remote(
                        outgoing.at[j], far_box.at[j], so.at[j], ro.at[j], "tensor", place.slot(j, 0)
                    )
                    copy.start()
                    item["far"][j] = copy
        for entry in plan:
            place = places[entry["axis"]]
            held = work[entry["held"]] if "held" in entry else outs[entry["out"]]
            so, ro, si, ri, own_sem = work[entry["sems"] : entry["sems"] + 5]
            for j in range(1, place.outer):
                entry["far"][j - 1].wait_recv()
                block = held.at[place.slot(-j, 0)]
                for k in range(1, place.inner):
                    at = j * (place.inner - 1) + k - 1
                    copy = remote(
                        block, block, si.at[at], ri.at[at], place.axis, place.slot(0, k)
                    )
                    copy.start()
                    entry["near"].append(copy)
            if "held" in entry:
                finish(entry, ins, outs, held)
        for item in sums:
            out = outs[item["out"]]
            far_box = work[item["scratch"] + 3]
            rows = out.shape[0]
            size = row_chunk(rows)
            for copy in item["far"].values():
                copy.wait_recv()

            @pl.loop(0, rows // size)
            def _(step, out=out, far_box=far_box, size=size, item=item):
                at = pl.ds(pl.multiple_of(step * size, size), size)
                value = out[at, :]
                for j in item["far"]:
                    value += far_box[j, at, :].astype(jnp.float32)
                out[at, :] = value

            for copy in [*item["near"].values(), *item["far"].values()]:
                copy.wait_send()
        for entry in plan:
            if "held" not in entry:
                for copy in entry["near"]:
                    copy.wait_recv()
                entry["own"].wait()
            for copy in entry["near"] + entry["far"]:
                copy.wait_send()

    def finish(entry, ins, outs, held):
        for copy in entry["near"]:
            copy.wait_recv()
        entry["own"].wait()
        count, rows, part = held.shape
        out = outs[entry["out"]]
        size = row_chunk(rows)

        @pl.loop(0, rows // size)
        def _(step):
            at = pl.ds(pl.multiple_of(step * size, size), size)
            if entry["kind"] == "rows":
                for n in range(count):
                    out[at, n * part : (n + 1) * part] = held[n, at, :].astype(out.dtype)
                return
            square = jnp.zeros((size, part), jnp.float32)
            for n in range(count):
                value = held[n, at, :].astype(jnp.float32)
                square += value * value
            scale = lax.rsqrt(
                jnp.sum(square, axis=1, keepdims=True) / (count * part) + NORM_EPS
            )
            outs[entry["out"] + 1][at, :] = scale
            gain_ref = ins[entry["gain"]]
            for n in range(count):
                cols = slice(n * part, (n + 1) * part)
                value = held[n, at, :].astype(jnp.float32)
                out[at, cols] = (value * scale * gain_ref[:, cols]).astype(out.dtype)

    return pl.pallas_call(
        kernel,
        name=name,
        out_shape=out_shapes,
        in_specs=in_specs,
        out_specs=out_specs,
        scratch_shapes=scratch,
        compiler_params=pltpu.CompilerParams(
            collective_id=number, has_side_effects=True, vmem_limit_bytes=VMEM_GRANT
        ),
    )(*operands)


def body(
    ref_hidden,
    pol_hidden,
    readout,
    lengths,
    pairing,
    pre_gain,
    post_gain,
    w_query,
    w_key,
    value_projection,
    w_out,
    a_query,
    a_value,
    query_second_factor,
    value_second_factor,
):
    f32, bf16 = jnp.float32, jnp.bfloat16
    tok_rows, part_width = pol_hidden.shape
    seqs_here = lengths.shape[0]
    length = tok_rows // seqs_here
    tensor_rank = lax.axis_index("tensor")
    data_rank = lax.axis_index("dp")
    counts = {"dp": lax.axis_size("dp"), "tensor": lax.axis_size("tensor")}
    all_seqs = seqs_here * counts["dp"]
    full_width = part_width * counts["tensor"]
    rank_size = query_second_factor.shape[0]
    rows_contraction = (((0,), (0,)), ((), ()))
    contract_cols = (((1,), (1,)), ((), ()))

    def dot(a, b, dims=(((1,), (0,)), ((), ()))):
        return lax.dot_general(a, b, dims, preferred_element_type=f32)

    pre_local = lax.dynamic_slice_in_dim(pre_gain, tensor_rank * part_width, part_width)
    post_local = lax.dynamic_slice_in_dim(post_gain, tensor_rank * part_width, part_width)
    hidden = jnp.concatenate([ref_hidden, pol_hidden], axis=0)
    gathered = communicate(
        "gather_inputs",
        1,
        counts,
        gathers=[
            (jnp.concatenate([a_query, a_value], axis=1), "dp", "hbm"),
            (w_query, "dp", "hbm"),
            (hidden, "tensor", "norm"),
            (w_key, "dp", "hbm"),
            (value_projection, "dp", "hbm"),
            (w_out, "dp", "hbm"),
        ],
        gain=pre_gain,
    )
    a_both, w_query_all, normed, pre_scale, w_key_all, w_value_all, w_out_all = [
        v.reshape(-1, v.shape[-1]) for v in gathered
    ]
    pol_normed = normed[tok_rows:]
    pol_scale = pre_scale[tok_rows:]
    low_rank_update = dot(pol_normed, a_both).astype(bf16)
    query_rows = dot(normed, w_query_all)
    keys_before_rotation = dot(normed, w_key_all)
    value_rows = dot(normed, w_value_all)
    added_query = ADAPTER_SCALE * dot(low_rank_update[:, :rank_size], query_second_factor)
    added_value = ADAPTER_SCALE * dot(low_rank_update[:, rank_size:], value_second_factor)
    none = ((tok_rows, 0), (0, 0))
    query_rows = query_rows + jnp.pad(added_query, none)
    value_rows = value_rows + jnp.pad(added_value, none)
    q_heads = query_rows.shape[1] // HEAD_SIZE
    kv_heads = value_rows.shape[1] // HEAD_SIZE
    both = 2 * seqs_here
    query_rows = apply_rotation(
        query_rows.reshape(both, length, q_heads, HEAD_SIZE), 1.0
    ).astype(bf16)
    rotated_keys = apply_rotation(
        keys_before_rotation.reshape(both, length, kv_heads, HEAD_SIZE), 1.0
    ).astype(bf16)
    value_rows = value_rows.reshape(both, length, kv_heads, HEAD_SIZE).astype(bf16)
    mixed_out, probs_low, probabilities, capped = attend(
        query_rows, rotated_keys, value_rows, jnp.concatenate([lengths, lengths])
    )
    head_terms = dot(
        mixed_out.reshape(2 * tok_rows, q_heads * HEAD_SIZE), w_out_all, contract_cols
    ).astype(bf16)
    (summed_both,) = communicate("scatter_out", 2, counts, reduces=[head_terms])
    readout_wide = readout.astype(f32)
    living = (jnp.arange(length)[None, :] < lengths[:, None]).astype(f32)
    weighted = post_local * readout_wide
    shaped = summed_both.reshape(2, tok_rows, part_width)
    hidden_wide = hidden.astype(f32).reshape(2, tok_rows, part_width)
    stats = jnp.concatenate(
        [
            jnp.sum(shaped * shaped, axis=2),
            jnp.sum(shaped * weighted, axis=2),
            jnp.sum(hidden_wide * readout_wide, axis=2),
            jnp.zeros((2, tok_rows), f32),
        ],
        axis=0,
    )
    (stats_all,) = communicate("token_sums", 3, counts, gathers=[(stats, "tensor", "vmem")])
    stats = jnp.sum(stats_all, axis=0)
    post_scale = lax.rsqrt(stats[0:2] / full_width + NORM_EPS)
    token_scores = (stats[4:6] + post_scale * stats[2:4]).reshape(2, seqs_here, length) * living
    mine = jnp.sum(token_scores, axis=2)
    mine = jnp.pad(mine, ((0, 6), (0, 128 - seqs_here)))
    (scores_all,) = communicate("sequence_scores", 4, counts, gathers=[(mine, "dp", "vmem")])
    scores = jnp.transpose(scores_all[:, :2, :seqs_here], (1, 0, 2)).reshape(2, all_seqs)
    ratios = scores[1] - scores[0]
    chooser = (pairing[:, None] == jnp.arange(all_seqs)[None, :]).astype(f32)
    picked = jnp.sum(chooser * ratios[None, :], axis=1).reshape(-1, 2)
    margins = DPO_BETA * (picked[:, 0] - picked[:, 1])
    dpo_loss = jnp.sum(jax.nn.softplus(-margins))
    pair_pull = DPO_BETA * LOSS_SCALE * jax.nn.sigmoid(-margins)
    signed = jnp.stack([-pair_pull, pair_pull], axis=1).reshape(-1)
    coefficients = jnp.sum(signed[:, None] * chooser, axis=0)
    local_coef = lax.dynamic_slice_in_dim(coefficients, data_rank * seqs_here, seqs_here)
    token_coef = (local_coef[:, None] * living).reshape(tok_rows)
    grad_result = token_coef[:, None] * readout_wide
    post_dot = token_coef * stats[3]
    summed = shaped[1]
    scale_col = post_scale[1][:, None]
    result = hidden_wide + shaped * post_scale[:, :, None] * post_local
    grad_summed = (
        scale_col * post_local * grad_result
        - summed * scale_col**3 * post_dot[:, None] / full_width
    ).astype(bf16)
    (grad_wide,) = communicate("gather_grad", 5, counts, gathers=[(grad_summed, "tensor", "rows")])
    grad_mixed = dot(grad_wide, w_out_all).astype(bf16)
    grad_q_rot, rotated_key_gradient, value_head_gradient = attend_back(
        grad_mixed.reshape(seqs_here, length, q_heads, HEAD_SIZE),
        query_rows[seqs_here:],
        rotated_keys[seqs_here:],
        value_rows[seqs_here:],
        probs_low[seqs_here:],
        probabilities[seqs_here:],
        capped[seqs_here:],
    )
    query_rows_gradient = apply_rotation(grad_q_rot, -1.0).reshape(tok_rows, -1).astype(bf16)
    key_rows_gradient = (
        apply_rotation(rotated_key_gradient, -1.0).reshape(tok_rows, -1).astype(bf16)
    )
    value_rows_gradient = value_head_gradient.reshape(tok_rows, -1).astype(bf16)
    factor_terms = ADAPTER_SCALE * jnp.concatenate(
        [
            dot(low_rank_update[:, :rank_size], query_rows_gradient, rows_contraction),
            dot(low_rank_update[:, rank_size:], value_rows_gradient, rows_contraction),
        ],
        axis=1,
    )
    hook_terms = ADAPTER_SCALE * jnp.concatenate(
        [
            dot(query_rows_gradient, query_second_factor, contract_cols),
            dot(value_rows_gradient, value_second_factor, contract_cols),
        ],
        axis=1,
    )
    hook_all, factor_all = communicate(
        "adapter_sums",
        6,
        counts,
        gathers=[
            (hook_terms.astype(bf16), "tensor", "vmem"),
            (factor_terms.astype(bf16), "dp", "vmem"),
        ],
    )
    factor_gradient = jnp.sum(factor_all.astype(f32), axis=0)
    query_factor_gradient = factor_gradient[:, : query_second_factor.shape[1]]
    value_factor_gradient = factor_gradient[:, query_second_factor.shape[1] :]
    hook = jnp.sum(hook_all.astype(f32), axis=0).astype(bf16)
    adapter_term = dot(pol_normed, hook, rows_contraction)
    slice_rows = full_width // (counts["dp"] * counts["tensor"])
    adapter_term = adapter_term.reshape(counts["dp"], counts["tensor"], slice_rows, -1)
    adapter_mine = lax.dynamic_index_in_dim(adapter_term, tensor_rank, 1, keepdims=False)
    input_terms = (
        dot(query_rows_gradient, w_query_all, contract_cols)
        + dot(key_rows_gradient, w_key_all, contract_cols)
        + dot(value_rows_gradient, w_value_all, contract_cols)
    ).astype(bf16)
    adapter_blocks, grad_normed = communicate(
        "scatter_grad",
        7,
        counts,
        gathers=[(adapter_mine.astype(bf16), "dp", "vmem")],
        reduces=[input_terms],
    )
    adapter_rows = jnp.sum(
        lax.dynamic_index_in_dim(adapter_blocks, data_rank, 1, keepdims=False).astype(f32), axis=0
    )
    a_local = lax.dynamic_slice_in_dim(a_both, tensor_rank * part_width, part_width)
    grad_normed = grad_normed + dot(hook, a_local, contract_cols)
    narrow = pol_hidden.astype(f32)
    pre_sums = jnp.sum(narrow * pre_local * grad_normed, axis=1)
    pre_sums = jnp.pad(pre_sums[None, :], ((0, 7), (0, 0)))
    adapter_all, pre_all = communicate(
        "last_sums",
        8,
        counts,
        gathers=[(adapter_rows.astype(bf16), "tensor", "vmem"), (pre_sums, "tensor", "vmem")],
    )
    grad_a = adapter_all.reshape(-1, adapter_all.shape[-1]).astype(f32)
    pre_dot = jnp.sum(pre_all[:, 0, :], axis=0)
    grad_hidden = (
        grad_result
        + pol_scale * pre_local * grad_normed
        - narrow * pol_scale**3 * pre_dot[:, None] / full_width
    )
    return (
        result[1].astype(bf16),
        result[0].astype(bf16),
        dpo_loss,
        grad_hidden.astype(bf16),
        grad_a,
        query_factor_gradient,
        value_factor_gradient,
    )


def solution(mesh):
    placed = (
        P("dp", "tensor"),
        P("dp", "tensor"),
        P("dp", "tensor"),
        P("dp"),
        P(),
        P(),
        P(),
        P("dp", "tensor"),
        P("dp", "tensor"),
        P("dp", "tensor"),
        P("dp", "tensor"),
        P("dp", None),
        P("dp", None),
        P(None, "tensor"),
        P(None, "tensor"),
    )
    return jax.shard_map(
        body,
        mesh=mesh,
        in_specs=placed,
        out_specs=(
            P("dp", "tensor"),
            P("dp", "tensor"),
            P(),
            P("dp", "tensor"),
            P("dp", None),
            P(None, "tensor"),
            P(None, "tensor"),
        ),
        check_vma=False,
    )
```

```python
import jax
import jax.numpy as jnp
from jax import lax
from jax.experimental import pallas as pl
from jax.experimental.pallas import tpu as pltpu
from jax.sharding import PartitionSpec as P

MODEL_WIDTH = 4608
HQ = 32
HEAD_SIZE = 128


NORM_EPS = 1e-06
SOFT_CAP = 50.0
ADAPTER_SCALE = 0.5
DPO_BETA = 0.5
LOSS_SCALE = 256.0
ROPE_BASE = 10000.0


def query_scale():
    return float(MODEL_WIDTH // HQ) ** (-0.5)


def apply_rotation(value_rows, direction):
    length = value_rows.shape[1]
    head_depth = value_rows.shape[3]
    middle = head_depth // 2
    spacing = ROPE_BASE ** (-2.0 * jnp.arange(middle, dtype=jnp.float32) / head_depth)
    angles = jnp.arange(length, dtype=jnp.float32)[:, None] * spacing[None, :]
    cosine = jnp.cos(angles)[None, :, None, :]
    sine_part = direction * jnp.sin(angles)[None, :, None, :]
    leading = value_rows[..., :middle]
    trailing = value_rows[..., middle:]
    return jnp.concatenate(
        [leading * cosine - trailing * sine_part, trailing * cosine + leading * sine_part], axis=-1
    )


def allowed_mask(lengths, length):
    places = jnp.arange(length)
    causal = places[None, :] <= places[:, None]
    living = places[None, :] < lengths[:, None]
    return causal[None, None, None, :, :] & living[:, None, None, None, :]


def attend(query_rows, rotated_keys, value_rows, lengths):
    seqs_here, length, q_heads, head_depth = query_rows.shape
    kv_heads = rotated_keys.shape[2]
    grouped_heads = query_rows.reshape(seqs_here, length, kv_heads, q_heads // kv_heads, head_depth)
    scores = (
        jnp.einsum(
            "sqkgd,spkd->skgqp", grouped_heads, rotated_keys, preferred_element_type=jnp.float32
        )
        * query_scale()
    )
    capped = SOFT_CAP * jnp.tanh(scores / SOFT_CAP)
    allowed = allowed_mask(lengths, length)
    weights = jnp.where(allowed, jnp.exp(capped), 0.0)
    probabilities = weights / jnp.sum(weights, axis=-1, keepdims=True)
    probs_low = probabilities.astype(jnp.bfloat16)
    mixed_out = jnp.einsum(
        "skgqp,spkd->sqkgd", probs_low, value_rows, preferred_element_type=jnp.float32
    )
    return (
        mixed_out.astype(jnp.bfloat16).reshape(seqs_here, length, q_heads, head_depth),
        probs_low,
        probabilities,
        capped,
    )


def attend_back(grad_mixed, query_rows, rotated_keys, value_rows, probs_low, probabilities, capped):
    seqs_here, length, q_heads, head_depth = query_rows.shape
    kv_heads = rotated_keys.shape[2]
    shape_five = (seqs_here, length, kv_heads, q_heads // kv_heads, head_depth)
    grouped_heads = query_rows.reshape(shape_five)
    grad_grouped = grad_mixed.reshape(shape_five)
    grad_probs = jnp.einsum(
        "sqkgd,spkd->skgqp", grad_grouped, value_rows, preferred_element_type=jnp.float32
    )
    value_rows_gradient = jnp.einsum(
        "skgqp,sqkgd->spkd", probs_low, grad_grouped, preferred_element_type=jnp.float32
    )
    centered = grad_probs - jnp.sum(grad_probs * probabilities, axis=-1, keepdims=True)
    grad_scores = (
        probabilities * centered * (1.0 - (capped / SOFT_CAP) ** 2) * query_scale()
    ).astype(jnp.bfloat16)
    query_rows_gradient = jnp.einsum(
        "skgqp,spkd->sqkgd", grad_scores, rotated_keys, preferred_element_type=jnp.float32
    ).reshape(seqs_here, length, q_heads, head_depth)
    key_rows_gradient = jnp.einsum(
        "skgqp,sqkgd->spkd", grad_scores, grouped_heads, preferred_element_type=jnp.float32
    )
    return (query_rows_gradient, key_rows_gradient, value_rows_gradient)


MESH = pl.DeviceIdType.MESH
VMEM_GRANT = 60 * 2**20


def grid_of(axis, count):
    if axis == "dp":
        inner = 2 if count % 2 == 0 else 1
    else:
        inner = 1
        while (inner * 2) ** 2 <= count and count % (inner * 2) == 0:
            inner *= 2
    return count // inner, inner


def row_chunk(rows):
    for size in (48, 32, 16):
        if rows % size == 0:
            return size
    return rows


def piece_rows(rows):
    for size in range(96, 0, -16):
        if rows % size == 0:
            return size
    return rows


class Place:
    def __init__(self, axis, count):
        self.axis = axis
        self.outer, self.inner = grid_of(axis, count)
        rank = lax.axis_index(axis)
        self.a = lax.div(rank, self.inner)
        self.b = lax.rem(rank, self.inner)
        self.rank = rank

    def out_at(self, j):
        return lax.rem(self.a + j + self.outer, self.outer)

    def in_at(self, k):
        return lax.rem(self.b + k + self.inner, self.inner)

    def slot(self, j, k):
        return self.out_at(j) * self.inner + self.in_at(k)

    def peers(self):
        return [self.slot(j, 0) for j in range(1, self.outer)] + [
            self.slot(0, k) for k in range(1, self.inner)
        ]


def remote(src, dst, send_sem, recv_sem, axis, rank):
    return pltpu.make_async_remote_copy(
        src_ref=src,
        dst_ref=dst,
        send_sem=send_sem,
        recv_sem=recv_sem,
        device_id={axis: rank},
        device_id_type=MESH,
    )


def communicate(name, number, counts, gathers=(), reduces=(), gain=None):
    places_used = sorted({axis for _, axis, _ in gathers} | ({"tensor"} if reduces else set()))
    tensor_count = counts["tensor"]
    operands, in_specs, out_shapes, out_specs, scratch = [], [], [], [], []
    vmem = pl.BlockSpec(memory_space=pltpu.VMEM)
    plan = []
    for array, axis, kind in gathers:
        operands.append(array)
        in_specs.append(vmem)
        whole = (counts[axis],) + array.shape
        outer, inner = grid_of(axis, counts[axis])
        entry = {"axis": axis, "kind": kind, "x": len(operands) - 1}
        if kind in ("vmem", "hbm"):
            entry["out"] = len(out_shapes)
            out_shapes.append(jax.ShapeDtypeStruct(whole, array.dtype))
            out_specs.append(vmem if kind == "vmem" else pl.BlockSpec(memory_space=pl.ANY))
        else:
            entry["held"] = len(scratch)
            scratch.append(pltpu.VMEM(whole, array.dtype))
            entry["out"] = len(out_shapes)
            out_shapes.append(
                jax.ShapeDtypeStruct((array.shape[0], array.shape[1] * counts[axis]), jnp.bfloat16)
            )
            out_specs.append(vmem)
            if kind == "norm":
                out_shapes.append(jax.ShapeDtypeStruct((array.shape[0], 1), jnp.float32))
                out_specs.append(vmem)
                entry["gain"] = len(operands)
                operands.append(gain.reshape(1, -1))
                in_specs.append(vmem)
        entry["sems"] = len(scratch)
        size = piece_rows(array.shape[0]) if "held" in entry else array.shape[0]
        entry["size"], entry["pieces"] = size, array.shape[0] // size
        n_outer = max(outer - 1, 1) * entry["pieces"]
        n_inner = max(outer * (inner - 1), 1) * entry["pieces"]
        scratch += [
            pltpu.SemaphoreType.DMA((n_outer,)),
            pltpu.SemaphoreType.DMA((n_outer,)),
            pltpu.SemaphoreType.DMA((n_inner,)),
            pltpu.SemaphoreType.DMA((n_inner,)),
            pltpu.SemaphoreType.DMA,
        ]
        plan.append(entry)
    sums = []
    for array in reduces:
        rows, width = array.shape
        outer, inner = grid_of("tensor", tensor_count)
        part = width // tensor_count
        size = piece_rows(rows)
        pieces = rows // size
        n_inner = max(outer * (inner - 1), 1)
        sums.append(
            {
                "x": len(operands),
                "out": len(out_shapes),
                "scratch": len(scratch),
                "size": size,
                "pieces": pieces,
            }
        )
        operands.append(array)
        in_specs.append(vmem)
        out_shapes.append(jax.ShapeDtypeStruct((rows, part), jnp.float32))
        out_specs.append(vmem)
        scratch += [
            pltpu.VMEM((tensor_count, rows, part), array.dtype),
            pltpu.VMEM((n_inner, rows, part), array.dtype),
            pltpu.VMEM((outer, rows, part), array.dtype),
            pltpu.VMEM((outer, rows, part), array.dtype),
            pltpu.SemaphoreType.DMA((n_inner * pieces,)),
            pltpu.SemaphoreType.DMA((n_inner * pieces,)),
            pltpu.SemaphoreType.DMA((outer * pieces,)),
            pltpu.SemaphoreType.DMA((outer * pieces,)),
        ]
    n_in, n_out = len(operands), len(out_shapes)

    def kernel(*refs):
        ins, outs, work = refs[:n_in], refs[n_in : n_in + n_out], refs[n_in + n_out :]
        places = {axis: Place(axis, counts[axis]) for axis in places_used}
        barrier = pltpu.get_barrier_semaphore()
        total = 0
        for axis, place in places.items():
            for peer in place.peers():
                pl.semaphore_signal(barrier, inc=1, device_id={axis: peer}, device_id_type=MESH)
                total += 1
        pl.semaphore_wait(barrier, total)
        for entry in plan:
            place = places[entry["axis"]]
            x = ins[entry["x"]]
            held = work[entry["held"]] if "held" in entry else outs[entry["out"]]
            so, ro, si, ri, own_sem = work[entry["sems"] : entry["sems"] + 5]
            entry["far"], entry["near"] = [], []
            mine = held.at[place.rank]
            for c in range(entry["pieces"]):
                rows = pl.ds(c * entry["size"], entry["size"])
                for j in range(1, place.outer):
                    at = c * (place.outer - 1) + j - 1
                    copy = remote(
                        x.at[rows],
                        mine.at[rows],
                        so.at[at],
                        ro.at[at],
                        place.axis,
                        place.slot(j, 0),
                    )
                    copy.start()
                    entry["far"].append(copy)
                for k in range(1, place.inner):
                    at = c * place.outer * (place.inner - 1) + k - 1
                    copy = remote(
                        x.at[rows],
                        mine.at[rows],
                        si.at[at],
                        ri.at[at],
                        place.axis,
                        place.slot(0, k),
                    )
                    copy.start()
                    entry["near"].append(copy)
            entry["own"] = pltpu.make_async_copy(x, mine, own_sem)
            entry["own"].start()
        for item in sums:
            place = places["tensor"]
            x = ins[item["x"]]
            stage, near_box, outgoing, far_box, si, ri, so, ro = work[
                item["scratch"] : item["scratch"] + 8
            ]
            part = stage.shape[2]
            size = row_chunk(item["size"])
            n_near = place.outer * (place.inner - 1)
            item["near"], item["far"] = {}, {}
            for c in range(item["pieces"]):

                @pl.loop(0, item["size"] // size)
                def _(step, c=c, x=x, stage=stage, part=part, size=size, item=item):
                    at = pl.ds(pl.multiple_of(c * item["size"] + step * size, size), size)
                    for n in range(tensor_count):
                        stage[n, at, :] = x[at, n * part : (n + 1) * part]

                rows = pl.ds(c * item["size"], item["size"])
                for j in [*range(1, place.outer), 0]:
                    for k in range(1, place.inner):
                        at = j * (place.inner - 1) + k - 1
                        copy = remote(
                            stage.at[place.slot(j, k), rows],
                            near_box.at[at, rows],
                            si.at[c * n_near + at],
                            ri.at[c * n_near + at],
                            "tensor",
                            place.slot(0, k),
                        )
                        copy.start()
                        item["near"][c, j, k] = copy
        for item in sums:
            place = places["tensor"]
            out = outs[item["out"]]
            stage, near_box, outgoing, far_box, si, ri, so, ro = work[
                item["scratch"] : item["scratch"] + 8
            ]
            size = row_chunk(item["size"])
            for c in range(item["pieces"]):
                rows = pl.ds(c * item["size"], item["size"])
                for j in [*range(1, place.outer), 0]:
                    for k in range(1, place.inner):
                        item["near"][c, j, k].wait_recv()

                    @pl.loop(0, item["size"] // size)
                    def _(step, c=c, j=j, item=item, size=size):
                        at = pl.ds(pl.multiple_of(c * item["size"] + step * size, size), size)
                        value = stage[place.slot(j, 0), at, :].astype(jnp.float32)
                        for k in range(1, place.inner):
                            value += near_box[j * (place.inner - 1) + k - 1, at, :].astype(
                                jnp.float32
                            )
                        if j:
                            outgoing[j, at, :] = value.astype(outgoing.dtype)
                        else:
                            out[at, :] = value

                    if j:
                        copy = remote(
                            outgoing.at[j, rows],
                            far_box.at[j, rows],
                            so.at[c * place.outer + j],
                            ro.at[c * place.outer + j],
                            "tensor",
                            place.slot(j, 0),
                        )
                        copy.start()
                        item["far"][c, j] = copy
        for entry in sorted(plan, key=lambda entry: "held" not in entry):
            place = places[entry["axis"]]
            held = work[entry["held"]] if "held" in entry else outs[entry["out"]]
            so, ro, si, ri, own_sem = work[entry["sems"] : entry["sems"] + 5]
            for c in range(entry["pieces"]):
                rows = pl.ds(c * entry["size"], entry["size"])
                for j in range(1, place.outer):
                    entry["far"][c * (place.outer - 1) + j - 1].wait_recv()
                    block = held.at[place.slot(-j, 0), rows]
                    for k in range(1, place.inner):
                        at = (c * place.outer + j) * (place.inner - 1) + k - 1
                        copy = remote(
                            block, block, si.at[at], ri.at[at], place.axis, place.slot(0, k)
                        )
                        copy.start()
                        entry["near"].append(copy)
        for entry in plan:
            if "held" in entry:
                finish(entry, ins, outs, work[entry["held"]])
        for item in sums:
            out = outs[item["out"]]
            far_box = work[item["scratch"] + 3]
            size = row_chunk(item["size"])
            outer = places["tensor"].outer
            for c in range(item["pieces"]):
                for j in range(1, outer):
                    item["far"][c, j].wait_recv()

                @pl.loop(0, item["size"] // size)
                def _(step, c=c, out=out, far_box=far_box, size=size, item=item):
                    at = pl.ds(pl.multiple_of(c * item["size"] + step * size, size), size)
                    value = out[at, :]
                    for j in range(1, outer):
                        value += far_box[j, at, :].astype(jnp.float32)
                    out[at, :] = value

            for copy in [*item["near"].values(), *item["far"].values()]:
                copy.wait_send()
        for entry in plan:
            if "held" not in entry:
                for copy in entry["near"]:
                    copy.wait_recv()
                entry["own"].wait()
            for copy in entry["near"] + entry["far"]:
                copy.wait_send()

    def finish(entry, ins, outs, held):
        for copy in entry["near"]:
            copy.wait_recv()
        entry["own"].wait()
        count, rows, part = held.shape
        out = outs[entry["out"]]
        size = row_chunk(rows)

        @pl.loop(0, rows // size)
        def _(step):
            at = pl.ds(pl.multiple_of(step * size, size), size)
            if entry["kind"] == "rows":
                for n in range(count):
                    out[at, n * part : (n + 1) * part] = held[n, at, :].astype(out.dtype)
                return
            square = jnp.zeros((size, part), jnp.float32)
            for n in range(count):
                value = held[n, at, :].astype(jnp.float32)
                square += value * value
            scale = lax.rsqrt(
                jnp.sum(square, axis=1, keepdims=True) / (count * part) + NORM_EPS
            )
            outs[entry["out"] + 1][at, :] = scale
            gain_ref = ins[entry["gain"]]
            for n in range(count):
                cols = slice(n * part, (n + 1) * part)
                value = held[n, at, :].astype(jnp.float32)
                out[at, cols] = (value * scale * gain_ref[:, cols]).astype(out.dtype)

    return pl.pallas_call(
        kernel,
        name=name,
        out_shape=out_shapes,
        in_specs=in_specs,
        out_specs=out_specs,
        scratch_shapes=scratch,
        compiler_params=pltpu.CompilerParams(
            collective_id=number, has_side_effects=True, vmem_limit_bytes=VMEM_GRANT
        ),
    )(*operands)


def body(
    ref_hidden,
    pol_hidden,
    readout,
    lengths,
    pairing,
    pre_gain,
    post_gain,
    w_query,
    w_key,
    value_projection,
    w_out,
    a_query,
    a_value,
    query_second_factor,
    value_second_factor,
):
    f32, bf16 = jnp.float32, jnp.bfloat16
    tok_rows, part_width = pol_hidden.shape
    seqs_here = lengths.shape[0]
    length = tok_rows // seqs_here
    tensor_rank = lax.axis_index("tensor")
    data_rank = lax.axis_index("dp")
    counts = {"dp": lax.axis_size("dp"), "tensor": lax.axis_size("tensor")}
    all_seqs = seqs_here * counts["dp"]
    full_width = part_width * counts["tensor"]
    rank_size = query_second_factor.shape[0]
    rows_contraction = (((0,), (0,)), ((), ()))
    contract_cols = (((1,), (1,)), ((), ()))

    def dot(a, b, dims=(((1,), (0,)), ((), ()))):
        return lax.dot_general(a, b, dims, preferred_element_type=f32)

    pre_local = lax.dynamic_slice_in_dim(pre_gain, tensor_rank * part_width, part_width)
    post_local = lax.dynamic_slice_in_dim(post_gain, tensor_rank * part_width, part_width)
    hidden = jnp.concatenate([ref_hidden, pol_hidden], axis=0)
    gathered = communicate(
        "gather_inputs",
        1,
        counts,
        gathers=[
            (jnp.concatenate([a_query, a_value], axis=1), "dp", "hbm"),
            (w_query, "dp", "hbm"),
            (hidden, "tensor", "norm"),
            (w_key, "dp", "hbm"),
            (value_projection, "dp", "hbm"),
            (w_out, "dp", "hbm"),
        ],
        gain=pre_gain,
    )
    a_both, w_query_all, normed, pre_scale, w_key_all, w_value_all, w_out_all = [
        v.reshape(-1, v.shape[-1]) for v in gathered
    ]
    pol_normed = normed[tok_rows:]
    pol_scale = pre_scale[tok_rows:]
    low_rank_update = dot(pol_normed, a_both).astype(bf16)
    query_rows = dot(normed, w_query_all)
    keys_before_rotation = dot(normed, w_key_all)
    value_rows = dot(normed, w_value_all)
    added_query = ADAPTER_SCALE * dot(low_rank_update[:, :rank_size], query_second_factor)
    added_value = ADAPTER_SCALE * dot(low_rank_update[:, rank_size:], value_second_factor)
    none = ((tok_rows, 0), (0, 0))
    query_rows = query_rows + jnp.pad(added_query, none)
    value_rows = value_rows + jnp.pad(added_value, none)
    q_heads = query_rows.shape[1] // HEAD_SIZE
    kv_heads = value_rows.shape[1] // HEAD_SIZE
    both = 2 * seqs_here
    query_rows = apply_rotation(
        query_rows.reshape(both, length, q_heads, HEAD_SIZE), 1.0
    ).astype(bf16)
    rotated_keys = apply_rotation(
        keys_before_rotation.reshape(both, length, kv_heads, HEAD_SIZE), 1.0
    ).astype(bf16)
    value_rows = value_rows.reshape(both, length, kv_heads, HEAD_SIZE).astype(bf16)
    mixed_out, probs_low, probabilities, capped = attend(
        query_rows, rotated_keys, value_rows, jnp.concatenate([lengths, lengths])
    )
    head_terms = dot(
        mixed_out.reshape(2 * tok_rows, q_heads * HEAD_SIZE), w_out_all, contract_cols
    ).astype(bf16)
    (summed_both,) = communicate("scatter_out", 2, counts, reduces=[head_terms])
    readout_wide = readout.astype(f32)
    living = (jnp.arange(length)[None, :] < lengths[:, None]).astype(f32)
    weighted = post_local * readout_wide
    shaped = summed_both.reshape(2, tok_rows, part_width)
    hidden_wide = hidden.astype(f32).reshape(2, tok_rows, part_width)
    stats = jnp.concatenate(
        [
            jnp.sum(shaped * shaped, axis=2),
            jnp.sum(shaped * weighted, axis=2),
            jnp.sum(hidden_wide * readout_wide, axis=2),
            jnp.zeros((2, tok_rows), f32),
        ],
        axis=0,
    )
    (stats_all,) = communicate("token_sums", 3, counts, gathers=[(stats, "tensor", "vmem")])
    stats = jnp.sum(stats_all, axis=0)
    post_scale = lax.rsqrt(stats[0:2] / full_width + NORM_EPS)
    token_scores = (stats[4:6] + post_scale * stats[2:4]).reshape(2, seqs_here, length) * living
    mine = jnp.sum(token_scores, axis=2)
    mine = jnp.pad(mine, ((0, 6), (0, 128 - seqs_here)))
    (scores_all,) = communicate("sequence_scores", 4, counts, gathers=[(mine, "dp", "vmem")])
    scores = jnp.transpose(scores_all[:, :2, :seqs_here], (1, 0, 2)).reshape(2, all_seqs)
    ratios = scores[1] - scores[0]
    chooser = (pairing[:, None] == jnp.arange(all_seqs)[None, :]).astype(f32)
    picked = jnp.sum(chooser * ratios[None, :], axis=1).reshape(-1, 2)
    margins = DPO_BETA * (picked[:, 0] - picked[:, 1])
    dpo_loss = jnp.sum(jax.nn.softplus(-margins))
    pair_pull = DPO_BETA * LOSS_SCALE * jax.nn.sigmoid(-margins)
    signed = jnp.stack([-pair_pull, pair_pull], axis=1).reshape(-1)
    coefficients = jnp.sum(signed[:, None] * chooser, axis=0)
    local_coef = lax.dynamic_slice_in_dim(coefficients, data_rank * seqs_here, seqs_here)
    token_coef = (local_coef[:, None] * living).reshape(tok_rows)
    grad_result = token_coef[:, None] * readout_wide
    post_dot = token_coef * stats[3]
    summed = shaped[1]
    scale_col = post_scale[1][:, None]
    result = hidden_wide + shaped * post_scale[:, :, None] * post_local
    grad_summed = (
        scale_col * post_local * grad_result
        - summed * scale_col**3 * post_dot[:, None] / full_width
    ).astype(bf16)
    (grad_wide,) = communicate("gather_grad", 5, counts, gathers=[(grad_summed, "tensor", "rows")])
    grad_mixed = dot(grad_wide, w_out_all).astype(bf16)
    grad_q_rot, rotated_key_gradient, value_head_gradient = attend_back(
        grad_mixed.reshape(seqs_here, length, q_heads, HEAD_SIZE),
        query_rows[seqs_here:],
        rotated_keys[seqs_here:],
        value_rows[seqs_here:],
        probs_low[seqs_here:],
        probabilities[seqs_here:],
        capped[seqs_here:],
    )
    query_rows_gradient = apply_rotation(grad_q_rot, -1.0).reshape(tok_rows, -1).astype(bf16)
    key_rows_gradient = (
        apply_rotation(rotated_key_gradient, -1.0).reshape(tok_rows, -1).astype(bf16)
    )
    value_rows_gradient = value_head_gradient.reshape(tok_rows, -1).astype(bf16)
    factor_terms = ADAPTER_SCALE * jnp.concatenate(
        [
            dot(low_rank_update[:, :rank_size], query_rows_gradient, rows_contraction),
            dot(low_rank_update[:, rank_size:], value_rows_gradient, rows_contraction),
        ],
        axis=1,
    )
    hook_terms = ADAPTER_SCALE * jnp.concatenate(
        [
            dot(query_rows_gradient, query_second_factor, contract_cols),
            dot(value_rows_gradient, value_second_factor, contract_cols),
        ],
        axis=1,
    )
    input_terms = (
        dot(query_rows_gradient, w_query_all, contract_cols)
        + dot(key_rows_gradient, w_key_all, contract_cols)
        + dot(value_rows_gradient, w_value_all, contract_cols)
    ).astype(bf16)
    hook_all, factor_all, grad_normed = communicate(
        "scatter_grad",
        6,
        counts,
        gathers=[
            (hook_terms.astype(bf16), "tensor", "vmem"),
            (factor_terms.astype(bf16), "dp", "vmem"),
        ],
        reduces=[input_terms],
    )
    factor_gradient = jnp.sum(factor_all.astype(f32), axis=0)
    query_factor_gradient = factor_gradient[:, : query_second_factor.shape[1]]
    value_factor_gradient = factor_gradient[:, query_second_factor.shape[1] :]
    hook = jnp.sum(hook_all.astype(f32), axis=0).astype(bf16)
    adapter_term = dot(pol_normed, hook, rows_contraction)
    slice_rows = full_width // (counts["dp"] * counts["tensor"])
    adapter_term = adapter_term.reshape(counts["dp"], counts["tensor"], slice_rows, -1)
    adapter_mine = lax.dynamic_index_in_dim(adapter_term, tensor_rank, 1, keepdims=False)
    a_local = lax.dynamic_slice_in_dim(a_both, tensor_rank * part_width, part_width)
    grad_normed = grad_normed + dot(hook, a_local, contract_cols)
    narrow = pol_hidden.astype(f32)
    pre_sums = jnp.sum(narrow * pre_local * grad_normed, axis=1)
    pre_sums = jnp.pad(pre_sums[None, :], ((0, 7), (0, 0)))
    adapter_blocks, pre_all = communicate(
        "adapter_parts",
        7,
        counts,
        gathers=[(adapter_mine.astype(bf16), "dp", "vmem"), (pre_sums, "tensor", "vmem")],
    )
    adapter_rows = jnp.sum(
        lax.dynamic_index_in_dim(adapter_blocks, data_rank, 1, keepdims=False).astype(f32), axis=0
    )
    (adapter_all,) = communicate(
        "adapter_gather", 8, counts, gathers=[(adapter_rows.astype(bf16), "tensor", "vmem")]
    )
    grad_a = adapter_all.reshape(-1, adapter_all.shape[-1]).astype(f32)
    pre_dot = jnp.sum(pre_all[:, 0, :], axis=0)
    grad_hidden = (
        grad_result
        + pol_scale * pre_local * grad_normed
        - narrow * pol_scale**3 * pre_dot[:, None] / full_width
    )
    return (
        result[1].astype(bf16),
        result[0].astype(bf16),
        dpo_loss,
        grad_hidden.astype(bf16),
        grad_a,
        query_factor_gradient,
        value_factor_gradient,
    )


def solution(mesh):
    placed = (
        P("dp", "tensor"),
        P("dp", "tensor"),
        P("dp", "tensor"),
        P("dp"),
        P(),
        P(),
        P(),
        P("dp", "tensor"),
        P("dp", "tensor"),
        P("dp", "tensor"),
        P("dp", "tensor"),
        P("dp", None),
        P("dp", None),
        P(None, "tensor"),
        P(None, "tensor"),
    )
    return jax.shard_map(
        body,
        mesh=mesh,
        in_specs=placed,
        out_specs=(
            P("dp", "tensor"),
            P("dp", "tensor"),
            P(),
            P("dp", "tensor"),
            P("dp", None),
            P(None, "tensor"),
            P(None, "tensor"),
        ),
        check_vma=False,
    )
```
